256 devices in a mesh: aa: 32 (over y, z_hi, x), ba: 2 (over core), col: 4 (over z_lo).
Axes of the slice: x: 4, y: 4, z: 8 (z_hi: 2, z_lo: 4; z = z_hi * 4 + z_lo), core: 2. Of those that a mesh axis runs over, the one named last changes fastest.
Arguments:
- tokens: bfloat16 [8192, 7168], P('aa', ('ba', 'col')), may hold values from -6 to 6
- expert_ids: int32 [8192, 8], P('aa'), may hold values from 0 to 383, as said below
- route_weight: float32 [8192, 8], P('aa'), may hold values from 0.5 to 2
- w_gate: bfloat16 [32, 7168, 2048], P('aa', None, ('ba', 'col')), may hold values from -0.0625 to 0.0625
- w_up: bfloat16 [32, 7168, 2048], P('aa', None, ('ba', 'col')), may hold values from -0.0625 to 0.0625
- w_down: bfloat16 [32, 2048, 7168], P('aa', ('ba', 'col')), may hold values from -0.125 to 0.125
Outputs:
- mixed: bfloat16 [8192, 7168], P('aa', ('ba', 'col'))
The draws below stay inside these ranges and needn't reach their ends.
Inputs may be any that keep to these rules, and one draw needn't show every extreme that they name: `expert_ids`: each row names 8 different experts.
All inputs are finite; a program needn't handle non-finite values.
Results may differ from the reference program's by a relative error of at most 0.015.
Values may be sent and summed in bfloat16 or wider, within the bound.
No kernel may reach another device: no remote copies, remote signals or barrier semaphores. Data moves between devices by JAX's collectives and lax.ppermute only.
A program may use at most 64 MiB of HBM per device.

```python
import jax
import jax.numpy as jnp
from jax import lax

D = 7168
FF = 2048
EXPERTS = 384
TOP = 8
TOK_AA = 256
CAP = 8
EXPERTS_COMPUTED = 32
TOKENS = 8192
N_AA = 32
N_BA = 2
N_COL = 4


def draw_expert_ids(key, part):
    first = jax.random.fold_in(key, 11)
    second = jax.random.fold_in(key, 23)
    even_share = jax.random.randint(first, (TOKENS, EXPERTS), 0, 2 ** 20, dtype=jnp.int32)
    expert_numbering = jnp.arange(EXPERTS, dtype=jnp.int32)
    expert_popularity = jax.random.randint(second, (EXPERTS,), 0, 4, dtype=jnp.int32)
    extra_logit = jnp.where(expert_numbering < EXPERTS_COMPUTED, expert_popularity * 2 ** 23, 0).astype(jnp.int32)
    router_logits = even_share * 1024 + expert_numbering[None, :] + extra_logit[None, :]
    picked = lax.top_k(router_logits, TOP)[1]
    return picked.astype(jnp.int32)


def steps_of(own_key, shape, shards, least, top_value):
    level = 1.0
    for dim, parts in shards:
        heights = jax.random.uniform(jax.random.fold_in(jax.random.fold_in(own_key, 6), dim), (parts,), jnp.float32, least / len(shards), top_value / len(shards))
        level = level * jnp.repeat(jnp.exp(heights), shape[dim] // parts).reshape((-1,) + (1,) * (len(shape) - 1 - dim))
    return level


def gaussian(stream_key, shape, spread, reach, split=(), kind=jnp.bfloat16):
    array = spread * jax.random.normal(stream_key, shape, jnp.float32)
    if split:
        array = array * steps_of(stream_key, shape, split, -0.22, 0.18)
    return jnp.clip(array, -reach, reach).astype(kind)


def setup_inputs(seed: int = 0) -> dict:
    key_of = jax.random.split(jax.random.key(seed), 7)
    tokens = gaussian(key_of[0], (TOKENS, D), 1.0, 6.0, ((0, 32), (1, 8)))
    expert_ids = draw_expert_ids(jax.random.fold_in(key_of[6], 71), 0)
    route_weight = jnp.clip(0.5 + 1.5 * jax.random.uniform(key_of[2], (TOKENS, TOP), jnp.float32) ** steps_of(key_of[2], (TOKENS, TOP), ((0, 32),), -0.2, 0.2), 0.5, 2.0)
    w_gate = gaussian(key_of[3], (EXPERTS_COMPUTED, D, FF), D ** -0.5, 0.0625, ((0, 32), (2, 8)))
    w_up = gaussian(key_of[4], (EXPERTS_COMPUTED, D, FF), D ** -0.5, 0.0625, ((0, 32), (2, 8)))
    w_down = gaussian(key_of[5], (EXPERTS_COMPUTED, FF, D), FF ** -0.5, 0.125, ((0, 32), (1, 8)))
    return {"tokens": tokens, "expert_ids": expert_ids, "route_weight": route_weight, "w_gate": w_gate, "w_up": w_up, "w_down": w_down}


def assign(group_ids):
    expert_pool = jnp.arange(EXPERTS_COMPUTED, dtype=jnp.int32)
    matched = group_ids[:, :, None] == expert_pool[None, None, :]
    counted = jnp.sum(matched.astype(jnp.int32), axis=1)
    before = jnp.cumsum(counted, axis=0) - counted
    retained = (counted > 0) & (before < CAP)
    placed = retained[:, :, None] & (before[:, :, None] == jnp.arange(CAP, dtype=jnp.int32)[None, None, :])
    positions = jnp.arange(TOK_AA, dtype=jnp.int32)[:, None, None]
    source_row = jnp.sum(jnp.where(placed, positions, 0), axis=0).astype(jnp.int32)
    filled = jnp.any(placed, axis=0)
    pick_slot = jnp.sum(jnp.where(matched, before[:, None, :], 0), axis=2).astype(jnp.int32)
    pick_kept = jnp.any(matched & retained[:, None, :], axis=2)
    return source_row, filled, pick_slot, pick_kept


def expert_ffn(operands):
    rows, gate_matrix, up_matrix, down_matrix = operands
    gate_sum = jnp.dot(rows, gate_matrix, preferred_element_type=jnp.float32)
    up_sum = jnp.dot(rows, up_matrix, preferred_element_type=jnp.float32)
    hidden = (jax.nn.silu(gate_sum) * up_sum).astype(jnp.bfloat16)
    blocks = N_BA * N_COL
    width = FF // blocks
    total = jnp.zeros((rows.shape[0], D), jnp.float32)
    for segment in range(blocks):
        partial_value = jnp.dot(hidden[:, segment * width:(segment + 1) * width],
                          down_matrix[segment * width:(segment + 1) * width],
                          preferred_element_type=jnp.float32).astype(jnp.bfloat16)
        partial_value = lax.optimization_barrier(partial_value)
        total = total + partial_value.astype(jnp.float32)
    return total.astype(jnp.bfloat16)


def reference(tokens, expert_ids, route_weight, w_gate, w_up, w_down):
    grouped = tokens.reshape(N_AA, TOK_AA, D)
    source_row, filled, pick_slot, pick_kept = jax.vmap(assign)(expert_ids.reshape(N_AA, TOK_AA, TOP))
    group_index = jnp.arange(N_AA, dtype=jnp.int32)[:, None, None]
    rows = grouped[group_index, source_row]
    rows = jnp.where(filled[:, :, :, None], rows, jnp.zeros_like(rows))
    per_expert = jnp.transpose(rows, (1, 0, 2, 3)).reshape(EXPERTS_COMPUTED, N_AA * CAP, D)
    outputs = lax.map(expert_ffn, (per_expert, w_gate, w_up, w_down)).reshape(EXPERTS_COMPUTED, N_AA, CAP, D)
    target = jnp.clip(expert_ids, 0, EXPERTS_COMPUTED - 1).astype(jnp.int32)
    slots = pick_slot.reshape(TOKENS, TOP)
    kept_flat = pick_kept.reshape(TOKENS, TOP)
    group_of = (jnp.arange(TOKENS, dtype=jnp.int32) // TOK_AA).astype(jnp.int32)
    weights = jnp.where(kept_flat, route_weight, jnp.zeros_like(route_weight))
    mixed = jnp.zeros((TOKENS, D), jnp.float32)
    for pick in range(TOP):
        chosen = outputs[target[:, pick], group_of, slots[:, pick]].astype(jnp.float32)
        mixed = mixed + weights[:, pick, None] * chosen
    return mixed.astype(jnp.bfloat16)
```

```python
import jax
import jax.numpy as jnp
from jax import lax
from jax.experimental import pallas as pl
from jax.experimental.pallas import tpu as pltpu
from jax.sharding import PartitionSpec as P

CAP = 8
F32 = jnp.float32
BF16 = jnp.bfloat16


def mm(a, b):
    return jnp.dot(a, b, preferred_element_type=F32)


def slots_of(ids, experts):
    top, tokens = ids.shape
    pool = lax.broadcasted_iota(jnp.int32, (experts, tokens), 0)
    hit = jnp.zeros((experts, tokens), F32)
    for k in range(top):
        hit = hit + jnp.where(ids[k : k + 1, :] == pool, 1.0, 0.0)
    earlier = lax.broadcasted_iota(jnp.int32, (tokens, tokens), 0)
    later = lax.broadcasted_iota(jnp.int32, (tokens, tokens), 1)
    before = mm(hit.astype(BF16), jnp.where(earlier < later, 1.0, 0.0).astype(BF16))
    rank = before.astype(jnp.int32)
    kept = (hit > 0.0) & (rank < CAP)
    rank = jnp.where(kept, rank, -1)
    return pool, rank


def placed_of(rank, value):
    experts, tokens = rank.shape
    slot = lax.broadcasted_iota(jnp.int32, (experts, CAP, tokens), 1)
    spread = lax.broadcast_in_dim(rank, (experts, CAP, tokens), (0, 2))
    filled = lax.broadcast_in_dim(value, (experts, CAP, tokens), (0, 2))
    return jnp.where(spread == slot, filled, 0.0).reshape(experts * CAP, tokens)


def dispatch_body(ids_ref, tok_ref, out_ref):
    experts, copies, cap, width = out_ref.shape
    _, rank = slots_of(ids_ref[...], experts)
    chooser = placed_of(rank, jnp.ones(rank.shape, F32)).astype(BF16)
    rows = mm(chooser, tok_ref[...]).astype(BF16).reshape(experts, cap, width)
    for j in range(copies):
        out_ref[:, j] = rows


def weights_body(ids_ref, rw_ref, high_ref, low_ref):
    ids = ids_ref[...]
    rw = rw_ref[...]
    pool, rank = slots_of(ids, high_ref.shape[1] // CAP)
    share = jnp.zeros(pool.shape, F32)
    for k in range(ids.shape[0]):
        share = share + jnp.where(ids[k : k + 1, :] == pool, rw[k : k + 1, :], 0.0)
    weight = placed_of(rank, share).T
    high = weight.astype(BF16)
    high_ref[...] = high
    low_ref[...] = (weight - high.astype(F32)).astype(BF16)


def first_body(b_ref, x_ref, wg_ref, wu_ref, g_ref, u_ref):
    x = x_ref[...].reshape(-1, x_ref.shape[3])

    @pl.when(pl.program_id(0) == 0)
    def _():
        g_ref[...] = jnp.zeros_like(g_ref)
        u_ref[...] = jnp.zeros_like(u_ref)

    g_ref[...] += mm(x, wg_ref[0])
    u_ref[...] += mm(x, wu_ref[0])


def second_body(b_ref, x_ref, wg_ref, wu_ref, g0_ref, u0_ref, wd_ref, h_ref, out_ref, g_ref, u_ref):
    step = pl.program_id(0)
    half = pl.num_programs(0) // 2

    @pl.when(step == 0)
    def _():
        g_ref[...] = g0_ref[...]
        u_ref[...] = u0_ref[...]

    @pl.when(step < half)
    def _():
        x = x_ref[...].reshape(-1, x_ref.shape[3])
        g_ref[...] += mm(x, wg_ref[0])
        u_ref[...] += mm(x, wu_ref[0])

    @pl.when(step == half - 1)
    def _():
        g = g_ref[...]
        h_ref[...] = (g / (1.0 + jnp.exp(-g)) * u_ref[...]).astype(BF16)

    @pl.when(step >= half)
    def _():
        out_ref[...] = mm(h_ref[...], wd_ref[...]).astype(BF16).reshape(out_ref.shape)


def third_body(b_ref, h_ref, wd_ref, r_ref, out_ref):
    own = mm(h_ref[...], wd_ref[...])
    other = r_ref[...].reshape(own.shape).astype(F32)
    out_ref[...] = (own + other).astype(BF16).reshape(out_ref.shape)


def combine_body(r_ref, high_ref, low_ref, out_ref):
    experts, copies, cap, width = r_ref.shape
    total = r_ref[:, 0].astype(F32)
    for j in range(1, copies):
        total = total + r_ref[:, j].astype(F32)
    rows = total.astype(BF16).reshape(experts * cap, width)
    out_ref[...] = (mm(high_ref[...], rows) + mm(low_ref[...], rows)).astype(BF16)


def shards(tokens, expert_ids, route_weight, w_gate, w_up, w_down):
    n_aa, n_ba, n_col = lax.axis_size("aa"), lax.axis_size("ba"), lax.axis_size("col")
    n_tok, width = tokens.shape
    hid = w_gate.shape[2]
    n_slot = n_aa * CAP
    ids = expert_ids.T
    rw = route_weight.T
    b = lax.axis_index("ba").astype(jnp.int32).reshape(1)
    wg = w_gate.reshape(n_ba * n_col, width, hid)
    wu = w_up.reshape(n_ba * n_col, width, hid)
    wd = w_down[0]
    swap = [(i, n_ba - 1 - i) for i in range(n_ba)]
    axes = ("aa", "col")
    big = jax.ShapeDtypeStruct((n_aa, n_col, CAP, width), BF16)
    block = (n_aa, 1, CAP, width)
    acc = jax.ShapeDtypeStruct((n_slot, hid), F32)
    whole = lambda shape: pl.BlockSpec(shape, lambda i, b: (0,) * len(shape))

    picked = pl.pallas_call(dispatch_body, out_shape=big, name="dispatch")(ids, tokens)
    mine = lax.all_to_all(picked.reshape(n_aa * n_col, CAP, width), axes, 0, 0, tiled=True)
    mine = mine.reshape(big.shape)
    theirs = lax.ppermute(mine, "ba", swap)

    g, u = pl.pallas_call(
        first_body,
        name="first",
        grid_spec=pltpu.PrefetchScalarGridSpec(
            num_scalar_prefetch=1,
            grid=(n_col,),
            in_specs=[
                pl.BlockSpec(block, lambda i, b: (0, i, 0, 0)),
                pl.BlockSpec((1, width, hid), lambda i, b: (b[0] * n_col + i, 0, 0)),
                pl.BlockSpec((1, width, hid), lambda i, b: (b[0] * n_col + i, 0, 0)),
            ],
            out_specs=[whole((n_slot, hid)), whole((n_slot, hid))],
        ),
        out_shape=[acc, acc],
    )(b, mine, wg, wu)

    last = n_col - 1
    w_at = lambda i, b: ((1 - b[0]) * n_col + jnp.minimum(i, last), 0, 0)
    hidden, sent = pl.pallas_call(
        second_body,
        name="second",
        grid_spec=pltpu.PrefetchScalarGridSpec(
            num_scalar_prefetch=1,
            grid=(2 * n_col,),
            in_specs=[
                pl.BlockSpec(block, lambda i, b: (0, jnp.minimum(i, last), 0, 0)),
                pl.BlockSpec((1, width, hid), w_at),
                pl.BlockSpec((1, width, hid), w_at),
                whole((n_slot, hid)),
                whole((n_slot, hid)),
                pl.BlockSpec((hid, width), lambda i, b: (0, (1 - b[0]) * n_col + jnp.maximum(i - n_col, 0))),
            ],
            out_specs=[
                whole((n_slot, hid)),
                pl.BlockSpec(block, lambda i, b: (0, jnp.maximum(i - n_col, 0), 0, 0)),
            ],
            scratch_shapes=[pltpu.VMEM((n_slot, hid), F32), pltpu.VMEM((n_slot, hid), F32)],
        ),
        out_shape=[jax.ShapeDtypeStruct((n_slot, hid), BF16), big],
    )(b, theirs, wg, wu, g, u, wd)

    got = lax.ppermute(sent, "ba", swap)
    pair = pl.pallas_call(
        third_body,
        name="third",
        grid_spec=pltpu.PrefetchScalarGridSpec(
            num_scalar_prefetch=1,
            grid=(n_col,),
            in_specs=[
                whole((n_slot, hid)),
                pl.BlockSpec((hid, width), lambda i, b: (0, b[0] * n_col + i)),
                pl.BlockSpec(block, lambda i, b: (0, i, 0, 0)),
            ],
            out_specs=pl.BlockSpec(block, lambda i, b: (0, i, 0, 0)),
        ),
        out_shape=big,
    )(b, hidden, wd, got)

    back = lax.all_to_all(pair.reshape(n_aa * n_col, CAP, width), axes, 0, 0, tiled=True)
    flat = jax.ShapeDtypeStruct((n_tok, n_slot), BF16)
    high, low = pl.pallas_call(weights_body, out_shape=[flat, flat], name="weights")(ids, rw)
    return pl.pallas_call(
        combine_body, out_shape=jax.ShapeDtypeStruct((n_tok, width), BF16), name="combine"
    )(back.reshape(big.shape), high, low)


def solution(mesh):
    in_specs = (
        P("aa", ("ba", "col")),
        P("aa", None),
        P("aa", None),
        P("aa", None, ("ba", "col")),
        P("aa", None, ("ba", "col")),
        P("aa", ("ba", "col"), None),
    )
    out_specs = P("aa", ("ba", "col"))
    return jax.shard_map(shards, mesh=mesh, in_specs=in_specs, out_specs=out_specs, check_vma=False)
```

```python
import jax
import jax.numpy as jnp
from jax import lax
from jax.experimental import pallas as pl
from jax.experimental.pallas import tpu as pltpu
from jax.sharding import PartitionSpec as P

CAP = 8
F32 = jnp.float32
BF16 = jnp.bfloat16


def held(x):
    return pltpu.with_memory_space_constraint(x, pltpu.VMEM)


def limit(mib):
    return pltpu.CompilerParams(vmem_limit_bytes=mib * 2**20)


def mm(a, b):
    return jnp.dot(a, b, preferred_element_type=F32)


def slots_of(ids, experts):
    top, tokens = ids.shape
    pool = lax.broadcasted_iota(jnp.int32, (experts, tokens), 0)
    hit = jnp.zeros((experts, tokens), F32)
    for k in range(top):
        hit = hit + jnp.where(ids[k : k + 1, :] == pool, 1.0, 0.0)
    earlier = lax.broadcasted_iota(jnp.int32, (tokens, tokens), 0)
    later = lax.broadcasted_iota(jnp.int32, (tokens, tokens), 1)
    before = mm(hit.astype(BF16), jnp.where(earlier < later, 1.0, 0.0).astype(BF16))
    rank = before.astype(jnp.int32)
    kept = (hit > 0.0) & (rank < CAP)
    rank = jnp.where(kept, rank, -1)
    return pool, rank


def placed_of(rank, value):
    experts, tokens = rank.shape
    slot = lax.broadcasted_iota(jnp.int32, (experts, CAP, tokens), 1)
    spread = lax.broadcast_in_dim(rank, (experts, CAP, tokens), (0, 2))
    filled = lax.broadcast_in_dim(value, (experts, CAP, tokens), (0, 2))
    return jnp.where(spread == slot, filled, 0.0).reshape(experts * CAP, tokens)


def prepare_body(ids_ref, rw_ref, tok_ref, out_ref, high_ref, low_ref):
    experts, copies, cap, width = out_ref.shape
    ids = ids_ref[...]
    rw = rw_ref[...]
    pool, rank = slots_of(ids, experts)
    chooser = placed_of(rank, jnp.ones(rank.shape, F32)).astype(BF16)
    rows = mm(chooser, tok_ref[...]).astype(BF16).reshape(experts, cap, width)
    for j in range(copies):
        out_ref[:, j] = rows
    share = jnp.zeros(pool.shape, F32)
    for k in range(ids.shape[0]):
        share = share + jnp.where(ids[k : k + 1, :] == pool, rw[k : k + 1, :], 0.0)
    weight = placed_of(rank, share).T
    high = weight.astype(BF16)
    high_ref[...] = high
    low_ref[...] = (weight - high.astype(F32)).astype(BF16)


def gate_up(x_ref, wg_ref, wu_ref, ready):
    copies, width = x_ref.shape[1], x_ref.shape[3]
    g = u = None
    for j in range(copies):
        ready(j)
        x = x_ref[:, j].reshape(-1, width)
        dg = mm(x, wg_ref[j])
        du = mm(x, wu_ref[j])
        g = dg if g is None else g + dg
        u = du if u is None else u + du
    return g, u


def first_body(b_ref, x_ref, wg_hbm, wu_hbm, wd_hbm, g_ref, u_ref, wg_ref, wu_ref, wd_ref, wg0_ref, wu0_ref, sems, late):
    b = b_ref[0]
    copies = x_ref.shape[1]
    near = [
        (
            pltpu.make_async_copy(wg_hbm.at[b * copies + j], wg0_ref.at[j], sems.at[j]),
            pltpu.make_async_copy(wu_hbm.at[b * copies + j], wu0_ref.at[j], sems.at[copies + j]),
        )
        for j in range(copies)
    ]
    far = [
        pltpu.make_async_copy(wg_hbm.at[pl.ds((1 - b) * copies, copies)], wg_ref, late.at[0]),
        pltpu.make_async_copy(wu_hbm.at[pl.ds((1 - b) * copies, copies)], wu_ref, late.at[1]),
        pltpu.make_async_copy(wd_hbm, wd_ref, late.at[2]),
    ]
    for pair in near:
        for move in pair:
            move.start()
    for move in far:
        move.start()

    def ready(j):
        for move in near[j]:
            move.wait()

    g_ref[...], u_ref[...] = gate_up(x_ref, wg0_ref, wu0_ref, ready)
    for move in far:
        move.wait()


def down(b, j, h, wd_ref, copies, width):
    at = pl.multiple_of((b * copies + j) * width, 128)
    return mm(h, wd_ref[:, pl.ds(at, width)])


def second_body(b_ref, x_ref, wg_ref, wu_ref, g_ref, u_ref, wd_ref, h_ref, out_ref):
    experts, copies, cap, width = x_ref.shape
    g, u = gate_up(x_ref, wg_ref, wu_ref, lambda j: None)
    g = g + g_ref[...]
    u = u + u_ref[...]
    h = (g / (1.0 + jnp.exp(-g)) * u).astype(BF16)
    h_ref[...] = h
    for j in range(copies):
        out_ref[:, j] = down(1 - b_ref[0], j, h, wd_ref, copies, width).astype(BF16).reshape(experts, cap, width)


def third_body(b_ref, h_ref, wd_ref, out_ref):
    experts, copies, cap, width = out_ref.shape
    h = h_ref[...]
    for j in range(copies):
        out_ref[:, j] = down(b_ref[0], j, h, wd_ref, copies, width).reshape(experts, cap, width)


def pair_body(own_ref, other_ref, out_ref):
    for j in range(out_ref.shape[1]):
        out_ref[:, j] = (own_ref[:, j] + other_ref[:, j].astype(F32)).astype(BF16)


def combine_body(r_ref, high_ref, low_ref, out_ref):
    experts, copies, cap, width = r_ref.shape
    total = r_ref[:, 0].astype(F32)
    for j in range(1, copies):
        total = total + r_ref[:, j].astype(F32)
    rows = total.astype(BF16).reshape(experts * cap, width)
    out_ref[...] = (mm(high_ref[...], rows) + mm(low_ref[...], rows)).astype(BF16)


def shards(tokens, expert_ids, route_weight, w_gate, w_up, w_down):
    n_aa, n_ba, n_col = lax.axis_size("aa"), lax.axis_size("ba"), lax.axis_size("col")
    n_tok, width = tokens.shape
    hid = w_gate.shape[2]
    n_slot = n_aa * CAP
    ids = expert_ids.T
    rw = route_weight.T
    b = lax.axis_index("ba").astype(jnp.int32).reshape(1)
    params = [w_gate.reshape(n_ba * n_col, width, hid), w_up.reshape(n_ba * n_col, width, hid), w_down[0]]
    swap = [(i, n_ba - 1 - i) for i in range(n_ba)]
    axes = ("aa", "col")
    shape = (n_aa, n_col, CAP, width)
    acc = pltpu.VMEM((n_slot, hid), F32)
    smem = pl.BlockSpec(memory_space=pltpu.SMEM)
    vmem = pl.BlockSpec(memory_space=pltpu.VMEM)

    hbm = pl.BlockSpec(memory_space=pl.ANY)
    flat = pltpu.VMEM((n_tok, n_slot), BF16)
    picked, high, low = pl.pallas_call(
        prepare_body,
        name="prepare",
        in_specs=[vmem] * 3,
        out_shape=[pltpu.VMEM(shape, BF16), flat, flat],
        out_specs=[vmem] * 3,
        compiler_params=limit(8),
    )(ids, rw, tokens)
    mine = lax.all_to_all(picked.reshape(n_aa * n_col, CAP, width), axes, 0, 0, tiled=True)
    mine = mine.reshape(shape)
    theirs = lax.ppermute(mine, "ba", swap)

    part = pltpu.VMEM((n_col, width, hid), BF16)
    g, u, wg, wu, wd = pl.pallas_call(
        first_body,
        name="first",
        in_specs=[smem, vmem] + [hbm] * 3,
        out_shape=[acc, acc, part, part, pltpu.VMEM(params[2].shape, BF16)],
        out_specs=[vmem] * 5,
        scratch_shapes=[part, part, pltpu.SemaphoreType.DMA((2 * n_col,)), pltpu.SemaphoreType.DMA((3,))],
        compiler_params=limit(16),
    )(b, held(mine), *[pltpu.with_memory_space_constraint(p, pltpu.HBM) for p in params])
    wg, wu, wd = held(wg), held(wu), held(wd)

    hidden, sent = pl.pallas_call(
        second_body,
        name="second",
        in_specs=[smem] + [vmem] * 6,
        out_shape=[pltpu.VMEM((n_slot, hid), BF16), pltpu.VMEM(shape, BF16)],
        compiler_params=limit(8),
    )(b, held(theirs), wg, wu, held(g), held(u), wd)

    got = lax.ppermute(sent, "ba", swap)
    own = pl.pallas_call(
        third_body,
        name="third",
        in_specs=[smem] + [vmem] * 2,
        out_shape=pltpu.VMEM(shape, F32),
        compiler_params=limit(8),
    )(b, held(hidden), wd)
    pair = pl.pallas_call(
        pair_body, name="pair", out_shape=pltpu.VMEM(shape, BF16), compiler_params=limit(8)
    )(held(own), held(got))

    back = lax.all_to_all(pair.reshape(n_aa * n_col, CAP, width), axes, 0, 0, tiled=True)
    return pl.pallas_call(
        combine_body,
        out_shape=jax.ShapeDtypeStruct((n_tok, width), BF16),
        name="combine",
        compiler_params=limit(8),
    )(held(back.reshape(shape)), held(high), held(low))


def solution(mesh):
    in_specs = (
        P("aa", ("ba", "col")),
        P("aa", None),
        P("aa", None),
        P("aa", None, ("ba", "col")),
        P("aa", None, ("ba", "col")),
        P("aa", ("ba", "col"), None),
    )
    out_specs = P("aa", ("ba", "col"))
    return jax.shard_map(shards, mesh=mesh, in_specs=in_specs, out_specs=out_specs, check_vma=False)
```

```python
import jax
import jax.numpy as jnp
from jax import lax
from jax.experimental import pallas as pl
from jax.experimental.pallas import tpu as pltpu
from jax.sharding import PartitionSpec as P

CAP = 8
F32 = jnp.float32
BF16 = jnp.bfloat16


def held(x):
    return pltpu.with_memory_space_constraint(x, pltpu.VMEM)


def far(x):
    return pltpu.with_memory_space_constraint(x, pltpu.HBM)


def limit(mib):
    return pltpu.CompilerParams(vmem_limit_bytes=mib * 2**20)


def mm(a, b):
    return jnp.dot(a, b, preferred_element_type=F32)


def slots_of(ids, experts):
    top, tokens = ids.shape
    pool = lax.broadcasted_iota(jnp.int32, (experts, tokens), 0)
    hit = jnp.zeros((experts, tokens), F32)
    for k in range(top):
        hit = hit + jnp.where(ids[k : k + 1, :] == pool, 1.0, 0.0)
    earlier = lax.broadcasted_iota(jnp.int32, (tokens, tokens), 0)
    later = lax.broadcasted_iota(jnp.int32, (tokens, tokens), 1)
    before = mm(hit.astype(BF16), jnp.where(earlier < later, 1.0, 0.0).astype(BF16))
    rank = before.astype(jnp.int32)
    kept = (hit > 0.0) & (rank < CAP)
    rank = jnp.where(kept, rank, -1)
    return pool, rank


def placed_of(rank, value):
    experts, tokens = rank.shape
    slot = lax.broadcasted_iota(jnp.int32, (experts, CAP, tokens), 1)
    spread = lax.broadcast_in_dim(rank, (experts, CAP, tokens), (0, 2))
    filled = lax.broadcast_in_dim(value, (experts, CAP, tokens), (0, 2))
    return jnp.where(spread == slot, filled, 0.0).reshape(experts * CAP, tokens)


def prepare_body(ids_hbm, rw_hbm, tok_hbm, out_ref, high_ref, low_ref, ids_ref, rw_ref, tok_ref, sems):
    experts, copies, cap, width = out_ref.shape
    moves = [
        pltpu.make_async_copy(ids_hbm, ids_ref, sems.at[0]),
        pltpu.make_async_copy(rw_hbm, rw_ref, sems.at[1]),
        pltpu.make_async_copy(tok_hbm, tok_ref, sems.at[2]),
    ]
    for move in moves:
        move.start()
    moves[0].wait()
    moves[1].wait()
    ids = ids_ref[...]
    rw = rw_ref[...]
    pool, rank = slots_of(ids, experts)
    chooser = placed_of(rank, jnp.ones(rank.shape, F32)).astype(BF16)
    share = jnp.zeros(pool.shape, F32)
    for k in range(ids.shape[0]):
        share = share + jnp.where(ids[k : k + 1, :] == pool, rw[k : k + 1, :], 0.0)
    weight = placed_of(rank, share).T
    high = weight.astype(BF16)
    high_ref[...] = high
    low_ref[...] = (weight - high.astype(F32)).astype(BF16)
    moves[2].wait()
    rows = mm(chooser, tok_ref[...]).astype(BF16).reshape(experts, cap, width)
    for j in range(copies):
        out_ref[:, j] = rows


def gate_up(x_ref, wg_ref, wu_ref, ready):
    copies, width = x_ref.shape[1], x_ref.shape[3]
    g = u = None
    for j in range(copies):
        ready(j)
        x = x_ref[:, j].reshape(-1, width)
        dg = mm(x, wg_ref[j])
        du = mm(x, wu_ref[j])
        g = dg if g is None else g + dg
        u = du if u is None else u + du
    return g, u


def first_body(b_ref, x_ref, wg_hbm, wu_hbm, g_ref, u_ref, wg_ref, wu_ref, wg0_ref, wu0_ref, sems, late):
    b = b_ref[0]
    copies = x_ref.shape[1]
    near = [
        (
            pltpu.make_async_copy(wg_hbm.at[b * copies + j], wg0_ref.at[j], sems.at[j]),
            pltpu.make_async_copy(wu_hbm.at[b * copies + j], wu0_ref.at[j], sems.at[copies + j]),
        )
        for j in range(copies)
    ]
    rest = [
        pltpu.make_async_copy(wg_hbm.at[pl.ds((1 - b) * copies, copies)], wg_ref, late.at[0]),
        pltpu.make_async_copy(wu_hbm.at[pl.ds((1 - b) * copies, copies)], wu_ref, late.at[1]),
    ]
    for pair in near:
        for move in pair:
            move.start()
    for move in rest:
        move.start()

    def ready(j):
        for move in near[j]:
            move.wait()

    g_ref[...], u_ref[...] = gate_up(x_ref, wg0_ref, wu0_ref, ready)
    for move in rest:
        move.wait()


def down(b, j, h, wd_ref, copies, width):
    at = pl.multiple_of((b * copies + j) * width, 128)
    return mm(h, wd_ref[:, pl.ds(at, width)])


def second_body(b_ref, x_hbm, wg_ref, wu_ref, g_ref, u_ref, wd_hbm, h_ref, out_ref, wd_ref, x_ref, sems):
    experts, copies, cap, width = x_ref.shape
    rows = [pltpu.make_async_copy(x_hbm.at[:, j], x_ref.at[:, j], sems.at[j]) for j in range(copies)]
    late = pltpu.make_async_copy(wd_hbm, wd_ref, sems.at[copies])
    for move in rows:
        move.start()
    late.start()
    g, u = gate_up(x_ref, wg_ref, wu_ref, lambda j: rows[j].wait())
    g = g + g_ref[...]
    u = u + u_ref[...]
    h = (g / (1.0 + jnp.exp(-g)) * u).astype(BF16)
    h_ref[...] = h
    late.wait()
    for j in range(copies):
        out_ref[:, j] = down(1 - b_ref[0], j, h, wd_ref, copies, width).astype(BF16).reshape(experts, cap, width)


def third_body(b_ref, h_ref, wd_ref, out_ref):
    experts, copies, cap, width = out_ref.shape
    h = h_ref[...]
    for j in range(copies):
        out_ref[:, j] = down(b_ref[0], j, h, wd_ref, copies, width).reshape(experts, cap, width)


def pair_body(own_ref, other_ref, out_ref):
    for j in range(out_ref.shape[1]):
        out_ref[:, j] = (own_ref[:, j] + other_ref[:, j].astype(F32)).astype(BF16)


def combine_body(r_ref, high_ref, low_ref, out_ref):
    experts, copies, cap, width = r_ref.shape
    total = r_ref[:, 0].astype(F32)
    for j in range(1, copies):
        total = total + r_ref[:, j].astype(F32)
    rows = total.astype(BF16).reshape(experts * cap, width)
    out_ref[...] = (mm(high_ref[...], rows) + mm(low_ref[...], rows)).astype(BF16)


def shards(tokens, expert_ids, route_weight, w_gate, w_up, w_down):
    n_aa, n_ba, n_col = lax.axis_size("aa"), lax.axis_size("ba"), lax.axis_size("col")
    n_tok, width = tokens.shape
    hid = w_gate.shape[2]
    n_slot = n_aa * CAP
    ids = expert_ids.T
    rw = route_weight.T
    b = lax.axis_index("ba").astype(jnp.int32).reshape(1)
    params = [w_gate.reshape(n_ba * n_col, width, hid), w_up.reshape(n_ba * n_col, width, hid), w_down[0]]
    swap = [(i, n_ba - 1 - i) for i in range(n_ba)]
    axes = ("aa", "col")
    shape = (n_aa, n_col, CAP, width)
    acc = pltpu.VMEM((n_slot, hid), F32)
    smem = pl.BlockSpec(memory_space=pltpu.SMEM)
    vmem = pl.BlockSpec(memory_space=pltpu.VMEM)

    hbm = pl.BlockSpec(memory_space=pl.ANY)
    flat = pltpu.VMEM((n_tok, n_slot), BF16)
    picked, high, low = pl.pallas_call(
        prepare_body,
        name="prepare",
        in_specs=[hbm] * 3,
        out_shape=[pltpu.VMEM(shape, BF16), flat, flat],
        out_specs=[vmem] * 3,
        scratch_shapes=[
            pltpu.VMEM(ids.shape, jnp.int32),
            pltpu.VMEM(rw.shape, F32),
            pltpu.VMEM(tokens.shape, BF16),
            pltpu.SemaphoreType.DMA((3,)),
        ],
        compiler_params=limit(8),
    )(far(ids), far(rw), far(tokens))
    mine = lax.all_to_all(picked.reshape(n_aa * n_col, CAP, width), axes, 0, 0, tiled=True)
    mine = mine.reshape(shape)
    theirs = lax.ppermute(mine, "ba", swap)

    part = pltpu.VMEM((n_col, width, hid), BF16)
    g, u, wg, wu = pl.pallas_call(
        first_body,
        name="first",
        in_specs=[smem, vmem] + [hbm] * 2,
        out_shape=[acc, acc, part, part],
        out_specs=[vmem] * 4,
        scratch_shapes=[part, part, pltpu.SemaphoreType.DMA((2 * n_col,)), pltpu.SemaphoreType.DMA((2,))],
        compiler_params=limit(16),
    )(b, held(mine), far(params[0]), far(params[1]))

    hidden, sent, wd = pl.pallas_call(
        second_body,
        name="second",
        in_specs=[smem, hbm] + [vmem] * 4 + [hbm],
        out_shape=[pltpu.VMEM((n_slot, hid), BF16), pltpu.VMEM(shape, BF16), pltpu.VMEM(params[2].shape, BF16)],
        out_specs=[vmem] * 3,
        scratch_shapes=[pltpu.VMEM(shape, BF16), pltpu.SemaphoreType.DMA((n_col + 1,))],
        compiler_params=limit(12),
    )(b, far(theirs), held(wg), held(wu), held(g), held(u), far(params[2]))

    got = lax.ppermute(sent, "ba", swap)
    own = pl.pallas_call(
        third_body,
        name="third",
        in_specs=[smem] + [vmem] * 2,
        out_shape=pltpu.VMEM(shape, F32),
        compiler_params=limit(8),
    )(b, held(hidden), held(wd))
    pair = pl.pallas_call(
        pair_body, name="pair", out_shape=pltpu.VMEM(shape, BF16), compiler_params=limit(8)
    )(held(own), held(got))

    back = lax.all_to_all(pair.reshape(n_aa * n_col, CAP, width), axes, 0, 0, tiled=True)
    return pl.pallas_call(
        combine_body,
        out_shape=jax.ShapeDtypeStruct((n_tok, width), BF16),
        name="combine",
        compiler_params=limit(8),
    )(held(back.reshape(shape)), held(high), held(low))


def solution(mesh):
    in_specs = (
        P("aa", ("ba", "col")),
        P("aa", None),
        P("aa", None),
        P("aa", None, ("ba", "col")),
        P("aa", None, ("ba", "col")),
        P("aa", ("ba", "col"), None),
    )
    out_specs = P("aa", ("ba", "col"))
    return jax.shard_map(shards, mesh=mesh, in_specs=in_specs, out_specs=out_specs, check_vma=False)
```

```python
import jax
import jax.numpy as jnp
from jax import lax
from jax.experimental import pallas as pl
from jax.experimental.pallas import tpu as pltpu
from jax.sharding import PartitionSpec as P

CAP = 8
F32 = jnp.float32
BF16 = jnp.bfloat16


def held(x):
    return pltpu.with_memory_space_constraint(x, pltpu.VMEM)


def far(x):
    return pltpu.with_memory_space_constraint(x, pltpu.HBM)


def limit(mib):
    return pltpu.CompilerParams(vmem_limit_bytes=mib * 2**20)


def mm(a, b):
    return jnp.dot(a, b, preferred_element_type=F32)


def slots_of(ids, experts):
    top, tokens = ids.shape
    pool = lax.broadcasted_iota(jnp.int32, (experts, tokens), 0)
    hit = jnp.zeros((experts, tokens), F32)
    for k in range(top):
        hit = hit + jnp.where(ids[k : k + 1, :] == pool, 1.0, 0.0)
    earlier = lax.broadcasted_iota(jnp.int32, (tokens, tokens), 0)
    later = lax.broadcasted_iota(jnp.int32, (tokens, tokens), 1)
    before = mm(hit.astype(BF16), jnp.where(earlier < later, 1.0, 0.0).astype(BF16))
    rank = before.astype(jnp.int32)
    kept = (hit > 0.0) & (rank < CAP)
    rank = jnp.where(kept, rank, -1)
    return pool, rank


def placed_of(rank, value):
    experts, tokens = rank.shape
    slot = lax.broadcasted_iota(jnp.int32, (experts, CAP, tokens), 1)
    spread = lax.broadcast_in_dim(rank, (experts, CAP, tokens), (0, 2))
    filled = lax.broadcast_in_dim(value, (experts, CAP, tokens), (0, 2))
    return jnp.where(spread == slot, filled, 0.0).reshape(experts * CAP, tokens)


def prepare_body(ids_hbm, rw_hbm, tok_hbm, out_hbm, high_ref, low_ref, ids_ref, rw_ref, tok_ref, rows_ref, sems, sent):
    experts, copies, cap, width = out_hbm.shape
    moves = [
        pltpu.make_async_copy(ids_hbm, ids_ref, sems.at[0]),
        pltpu.make_async_copy(rw_hbm, rw_ref, sems.at[1]),
        pltpu.make_async_copy(tok_hbm, tok_ref, sems.at[2]),
    ]
    for move in moves:
        move.start()
    moves[0].wait()
    ids = ids_ref[...]
    pool, rank = slots_of(ids, experts)
    chooser = placed_of(rank, jnp.ones(rank.shape, F32)).astype(BF16)
    moves[2].wait()
    rows_ref[...] = mm(chooser, tok_ref[...]).astype(BF16).reshape(experts, cap, width)
    out = [pltpu.make_async_copy(rows_ref, out_hbm.at[:, j], sent.at[j]) for j in range(copies)]
    for move in out:
        move.start()
    moves[1].wait()
    rw = rw_ref[...]
    share = jnp.zeros(pool.shape, F32)
    for k in range(ids.shape[0]):
        share = share + jnp.where(ids[k : k + 1, :] == pool, rw[k : k + 1, :], 0.0)
    weight = placed_of(rank, share).T
    high = weight.astype(BF16)
    high_ref[...] = high
    low_ref[...] = (weight - high.astype(F32)).astype(BF16)
    for move in out:
        move.wait()


def gate_up(b_ref, x_ref, wg_hbm, wu_hbm, wg_ref, wu_ref, sems):
    copies, width = x_ref.shape[1], x_ref.shape[3]
    at = b_ref[0] * copies
    moves = [
        (
            pltpu.make_async_copy(wg_hbm.at[at + j], wg_ref.at[j], sems.at[j]),
            pltpu.make_async_copy(wu_hbm.at[at + j], wu_ref.at[j], sems.at[copies + j]),
        )
        for j in range(copies)
    ]
    for pair in moves:
        for move in pair:
            move.start()
    g = u = None
    for j in range(copies):
        x = x_ref[:, j].reshape(-1, width)
        moves[j][0].wait()
        dg = mm(x, wg_ref[j])
        moves[j][1].wait()
        du = mm(x, wu_ref[j])
        g = dg if g is None else g + dg
        u = du if u is None else u + du
    return g, u


def sums_body(b_ref, x_ref, wg_hbm, wu_hbm, out_ref, wg_ref, wu_ref, sems):
    out_ref[0], out_ref[1] = gate_up(b_ref, x_ref, wg_hbm, wu_hbm, wg_ref, wu_ref, sems)


def hidden_body(own_ref, other_ref, out_ref):
    g = own_ref[0] + other_ref[0]
    u = own_ref[1] + other_ref[1]
    out_ref[...] = (g / (1.0 + jnp.exp(-g)) * u).astype(BF16)


def near_body(b_ref, h_ref, mine_hbm, theirs_hbm, out_ref, late_ref, w_ref, sems):
    experts, copies, cap, width = out_ref.shape
    moves = []
    for n, (hbm, ref) in enumerate(((mine_hbm, w_ref), (theirs_hbm, late_ref))):
        for j in range(copies):
            at = pl.multiple_of((b_ref[0] * copies + j) * width, 128)
            moves.append(pltpu.make_async_copy(hbm.at[:, pl.ds(at, width)], ref.at[j], sems.at[n * copies + j]))
    for move in moves:
        move.start()
    h = h_ref[...]
    for j in range(copies):
        moves[j].wait()
        out_ref[:, j] = mm(h, w_ref[j]).reshape(experts, cap, width)
    for j in range(copies):
        moves[copies + j].wait()


def far_body(h_ref, w_ref, own_ref, out_ref):
    experts, copies, cap, width = out_ref.shape
    h = h_ref[...]
    for j in range(copies):
        other = mm(h, w_ref[j]).reshape(experts, cap, width)
        out_ref[:, j] = (own_ref[:, j] + other).astype(BF16)


def combine_body(r_ref, high_ref, low_ref, out_ref):
    experts, copies, cap, width = r_ref.shape
    total = r_ref[:, 0].astype(F32)
    for j in range(1, copies):
        total = total + r_ref[:, j].astype(F32)
    rows = total.astype(BF16).reshape(experts * cap, width)
    out_ref[...] = (mm(high_ref[...], rows) + mm(low_ref[...], rows)).astype(BF16)


def shards(tokens, expert_ids, route_weight, w_gate, w_up, w_down):
    n_aa, n_ba, n_col = lax.axis_size("aa"), lax.axis_size("ba"), lax.axis_size("col")
    n_tok, width = tokens.shape
    hid = w_gate.shape[2]
    n_slot = n_aa * CAP
    ids = expert_ids.T
    rw = route_weight.T
    b = lax.axis_index("ba").astype(jnp.int32).reshape(1)
    params = [w_gate.reshape(n_ba * n_col, width, hid), w_up.reshape(n_ba * n_col, width, hid), w_down[0]]
    swap = [(i, n_ba - 1 - i) for i in range(n_ba)]
    axes = ("aa", "col")
    swapped = [lax.ppermute(p, "ba", swap) for p in params]
    shape = (n_aa, n_col, CAP, width)
    smem = pl.BlockSpec(memory_space=pltpu.SMEM)
    vmem = pl.BlockSpec(memory_space=pltpu.VMEM)

    hbm = pl.BlockSpec(memory_space=pl.ANY)
    flat = pltpu.VMEM((n_tok, n_slot), BF16)
    picked, high, low = pl.pallas_call(
        prepare_body,
        name="prepare",
        in_specs=[hbm] * 3,
        out_shape=[pltpu.HBM(shape, BF16), flat, flat],
        out_specs=[hbm, vmem, vmem],
        scratch_shapes=[
            pltpu.VMEM(ids.shape, jnp.int32),
            pltpu.VMEM(rw.shape, F32),
            pltpu.VMEM(tokens.shape, BF16),
            pltpu.VMEM((n_aa, CAP, width), BF16),
            pltpu.SemaphoreType.DMA((3,)),
            pltpu.SemaphoreType.DMA((n_col,)),
        ],
        compiler_params=limit(8),
    )(far(ids), far(rw), far(tokens))
    mine = lax.all_to_all(picked.reshape(n_aa * n_col, CAP, width), axes, 0, 0, tiled=True)
    mine = mine.reshape(shape)

    part = pltpu.VMEM((n_col, width, hid), BF16)
    sums = lambda name, gate, up: pl.pallas_call(
        sums_body,
        name=name,
        in_specs=[smem, vmem, hbm, hbm],
        out_shape=pltpu.VMEM((2, n_slot, hid), F32),
        out_specs=vmem,
        scratch_shapes=[part, part, pltpu.SemaphoreType.DMA((2 * n_col,))],
        compiler_params=limit(12),
    )(b, held(mine), far(gate), far(up))
    sent = sums("cross", swapped[0], swapped[1])
    got = lax.ppermute(sent, "ba", swap)
    own = sums("own", params[0], params[1])
    hidden = pl.pallas_call(
        hidden_body, name="hidden", out_shape=pltpu.VMEM((n_slot, hid), BF16), compiler_params=limit(8)
    )(held(own), held(got))
    other = lax.ppermute(hidden, "ba", swap)

    half = pltpu.VMEM((n_col, hid, width), BF16)
    near, late = pl.pallas_call(
        near_body,
        name="near",
        in_specs=[smem, vmem, hbm, hbm],
        out_shape=[pltpu.VMEM(shape, F32), half],
        out_specs=[vmem] * 2,
        scratch_shapes=[half, pltpu.SemaphoreType.DMA((2 * n_col,))],
        compiler_params=limit(12),
    )(b, held(hidden), far(params[2]), far(swapped[2]))
    pair = pl.pallas_call(
        far_body, name="far", out_shape=pltpu.VMEM(shape, BF16), compiler_params=limit(8)
    )(held(other), held(late), held(near))

    back = lax.all_to_all(pair.reshape(n_aa * n_col, CAP, width), axes, 0, 0, tiled=True)
    return pl.pallas_call(
        combine_body,
        out_shape=jax.ShapeDtypeStruct((n_tok, width), BF16),
        name="combine",
        compiler_params=limit(8),
    )(held(back.reshape(shape)), held(high), held(low))


def solution(mesh):
    in_specs = (
        P("aa", ("ba", "col")),
        P("aa", None),
        P("aa", None),
        P("aa", None, ("ba", "col")),
        P("aa", None, ("ba", "col")),
        P("aa", ("ba", "col"), None),
    )
    out_specs = P("aa", ("ba", "col"))
    return jax.shard_map(shards, mesh=mesh, in_specs=in_specs, out_specs=out_specs, check_vma=False)
```

```python
import functools

import jax
import jax.numpy as jnp
from jax import lax
from jax.experimental import pallas as pl
from jax.experimental.pallas import tpu as pltpu
from jax.sharding import PartitionSpec as P

CAP = 8
F32 = jnp.float32
BF16 = jnp.bfloat16


def held(x):
    return pltpu.with_memory_space_constraint(x, pltpu.VMEM)


def far(x):
    return pltpu.with_memory_space_constraint(x, pltpu.HBM)


def limit(mib):
    return pltpu.CompilerParams(vmem_limit_bytes=mib * 2**20)


def mm(a, b):
    return jnp.dot(a, b, preferred_element_type=F32)


def slots_of(ids, experts):
    top, tokens = ids.shape
    pool = lax.broadcasted_iota(jnp.int32, (experts, tokens), 0)
    hit = jnp.zeros((experts, tokens), F32)
    for k in range(top):
        hit = hit + jnp.where(ids[k : k + 1, :] == pool, 1.0, 0.0)
    earlier = lax.broadcasted_iota(jnp.int32, (tokens, tokens), 0)
    later = lax.broadcasted_iota(jnp.int32, (tokens, tokens), 1)
    before = mm(hit.astype(BF16), jnp.where(earlier < later, 1.0, 0.0).astype(BF16))
    rank = before.astype(jnp.int32)
    kept = (hit > 0.0) & (rank < CAP)
    rank = jnp.where(kept, rank, -1)
    return pool, rank


def placed_of(rank, value):
    experts, tokens = rank.shape
    slot = lax.broadcasted_iota(jnp.int32, (experts, CAP, tokens), 1)
    spread = lax.broadcast_in_dim(rank, (experts, CAP, tokens), (0, 2))
    filled = lax.broadcast_in_dim(value, (experts, CAP, tokens), (0, 2))
    return jnp.where(spread == slot, filled, 0.0).reshape(experts * CAP, tokens)


def dispatch_body(zh_ref, ids_hbm, tok_hbm, out_ref, ids_ref, tok_ref, rows_ref, sems):
    experts = out_ref.shape[0] * out_ref.shape[1] * out_ref.shape[2]
    moves = [pltpu.make_async_copy(ids_hbm, ids_ref, sems.at[0]), pltpu.make_async_copy(tok_hbm, tok_ref, sems.at[1])]
    for move in moves:
        move.start()
    moves[0].wait()
    _, rank = slots_of(ids_ref[...], experts)
    chooser = placed_of(rank, jnp.ones(rank.shape, F32)).astype(BF16)
    moves[1].wait()
    rows_ref[...] = mm(chooser, tok_ref[...]).astype(BF16).reshape(rows_ref.shape)
    for f in range(2):
        out_ref[:, :, f] = rows_ref[:, zh_ref[0] ^ f]


def split_body(x_ref, *out_refs):
    for f, ref in enumerate(out_refs):
        ref[...] = x_ref[:, f]


def weights_body(ids_ref, rw_ref, high_ref, low_ref):
    ids = ids_ref[...]
    rw = rw_ref[...]
    pool, rank = slots_of(ids, high_ref.shape[1] // CAP)
    share = jnp.zeros(pool.shape, F32)
    for k in range(ids.shape[0]):
        share = share + jnp.where(ids[k : k + 1, :] == pool, rw[k : k + 1, :], 0.0)
    weight = placed_of(rank, share).T
    high = weight.astype(BF16)
    high_ref[...] = high
    low_ref[...] = (weight - high.astype(F32)).astype(BF16)


def rows_of(x_refs):
    return jnp.concatenate([ref[...].reshape(-1, ref.shape[2]) for ref in x_refs], axis=0)


def first_body(d, blk_ref, x0_ref, x1_ref, wg_hbm, wu_hbm, og_hbm, ou_hbm, out_ref, w_ref, sems):
    stacks = (wg_hbm, wu_hbm, og_hbm, ou_hbm)
    moves = [pltpu.make_async_copy(hbm.at[blk_ref[d]], w_ref.at[n], sems.at[n]) for n, hbm in enumerate(stacks)]
    for move in moves:
        move.start()
    x = rows_of((x0_ref, x1_ref))
    for n, move in enumerate(moves):
        move.wait()
        out_ref[n] = mm(x, w_ref[n])


def second_body(
    ds, blk_ref, b_ref, x0_ref, x1_ref, acc_ref, wg_hbm, wu_hbm, og_hbm, ou_hbm, mine_hbm, theirs_hbm,
    out_ref, w1_ref, w2_ref, wn_ref, wf_ref, w_ref, sems, late,
):
    copies, _, width = wn_ref.shape
    stacks = (wg_hbm, wu_hbm, og_hbm, ou_hbm)
    moves = [pltpu.make_async_copy(hbm.at[blk_ref[ds[0]]], w_ref.at[n], sems.at[n]) for n, hbm in enumerate(stacks)]
    rest = []
    for d, ref in ((ds[1], w1_ref), (ds[2], w2_ref)):
        for n, hbm in enumerate(stacks):
            rest.append(pltpu.make_async_copy(hbm.at[blk_ref[d]], ref.at[n], late.at[len(rest)]))
    for hbm, ref in ((mine_hbm, wn_ref), (theirs_hbm, wf_ref)):
        for j in range(copies):
            at = pl.multiple_of((b_ref[0] * copies + j) * width, 128)
            rest.append(pltpu.make_async_copy(hbm.at[:, pl.ds(at, width)], ref.at[j], late.at[len(rest)]))
    for move in moves + rest:
        move.start()
    x = rows_of((x0_ref, x1_ref))
    for n, move in enumerate(moves):
        move.wait()
        out_ref[n] = acc_ref[n] + mm(x, w_ref[n])
    for move in rest:
        move.wait()


def third_body(x0_ref, x1_ref, w_ref, acc_ref, out_ref):
    x = rows_of((x0_ref, x1_ref))
    for n in range(out_ref.shape[0]):
        out_ref[n] = acc_ref[n] + mm(x, w_ref[n])


def last_body(at, x0_ref, x1_ref, w_ref, acc_ref, out_ref):
    x = rows_of((x0_ref, x1_ref))
    for n in range(out_ref.shape[0]):
        out_ref[n] = acc_ref[at + n] + mm(x, w_ref[at + n])


def hidden_body(own_ref, other_ref, out_ref):
    g = own_ref[0] + other_ref[0]
    u = own_ref[1] + other_ref[1]
    out_ref[...] = (g / (1.0 + jnp.exp(-g)) * u).astype(BF16)


def near_body(h_ref, w_ref, out_ref):
    shape = out_ref.shape[:3] + out_ref.shape[4:]
    h = h_ref[...]
    for j in range(out_ref.shape[3]):
        out_ref[:, :, :, j] = mm(h, w_ref[j]).reshape(shape)


def far_body(zh_ref, h_ref, w_ref, own_ref, out_ref):
    shape = own_ref.shape[:3] + own_ref.shape[4:]
    h = h_ref[...]
    for j in range(own_ref.shape[3]):
        total = (own_ref[:, :, :, j] + mm(h, w_ref[j]).reshape(shape)).astype(BF16)
        for f in range(2):
            out_ref[:, zh_ref[0] ^ f, :, j] = total[f]


def combine_body(r_ref, high_ref, low_ref, out_ref):
    experts, copies, cap, width = r_ref.shape
    total = r_ref[:, 0].astype(F32)
    for j in range(1, copies):
        total = total + r_ref[:, j].astype(F32)
    rows = total.astype(BF16).reshape(experts * cap, width)
    out_ref[...] = (mm(high_ref[...], rows) + mm(low_ref[...], rows)).astype(BF16)


def shards(tokens, expert_ids, route_weight, w_gate, w_up, w_down):
    n_aa, n_ba, n_col = lax.axis_size("aa"), lax.axis_size("ba"), lax.axis_size("col")
    n_tok, width = tokens.shape
    hid = w_gate.shape[2]
    n_slot = n_aa * CAP
    ids = expert_ids.T
    rw = route_weight.T
    b = lax.axis_index("ba").astype(jnp.int32).reshape(1)
    params = [w_gate.reshape(n_ba * n_col, width, hid), w_up.reshape(n_ba * n_col, width, hid), w_down[0]]
    swap = [(i, n_ba - 1 - i) for i in range(n_ba)]
    axes = ("aa", "col")
    shape = (n_aa, n_col, CAP, width)
    smem = pl.BlockSpec(memory_space=pltpu.SMEM)
    vmem = pl.BlockSpec(memory_space=pltpu.VMEM)

    hbm = pl.BlockSpec(memory_space=pl.ANY)
    ny, nh, nx = 4, 2, 4
    zh = ((lax.axis_index("aa") // nx) % nh).astype(jnp.int32).reshape(1)
    zl = lax.axis_index("col").astype(jnp.int32)
    blocks = b * n_col + (zl - jnp.arange(n_col, dtype=jnp.int32)) % n_col
    plane = [[(y * nh + h) * nx + x for y in range(ny) for x in range(nx)] for h in range(nh)]
    place = lambda y, h, x, l: ((y * nh + h) * nx + x) * n_col + l
    hop = lambda f, d: [
        (place(y, h, x, l), place(y, h ^ f, x, (l + d) % n_col))
        for y in range(ny)
        for h in range(nh)
        for x in range(nx)
        for l in range(n_col)
    ]

    picked = pl.pallas_call(
        dispatch_body,
        name="dispatch",
        in_specs=[smem] + [hbm] * 2,
        out_shape=pltpu.VMEM((ny, nx, nh, CAP, width), BF16),
        out_specs=vmem,
        scratch_shapes=[
            pltpu.VMEM(ids.shape, jnp.int32),
            pltpu.VMEM(tokens.shape, BF16),
            pltpu.VMEM((ny, nh, nx, CAP, width), BF16),
            pltpu.SemaphoreType.DMA((2,)),
        ],
        compiler_params=limit(8),
    )(zh, far(ids), far(tokens))
    swapped = [lax.ppermute(p, "ba", swap) for p in params]
    mine = lax.all_to_all(
        picked.reshape(ny * nx, nh, CAP, width), "aa", 0, 0, tiled=True, axis_index_groups=plane
    )
    flat = pltpu.VMEM((n_tok, n_slot), BF16)
    high, low = pl.pallas_call(weights_body, out_shape=[flat, flat], name="weights", compiler_params=limit(8))(ids, rw)
    piece = jax.ShapeDtypeStruct((ny * nx, CAP, width), BF16)
    sides = pl.pallas_call(split_body, name="split", out_shape=[piece] * nh, compiler_params=limit(8))(mine)
    got = {(0, 0): sides[0]}
    for f, d in [(1, 0)] + [(f, d) for d in range(1, n_col) for f in range(nh)]:
        got[f, d] = lax.ppermute(sides[f], axes, hop(f, d))

    four = pltpu.VMEM((4, n_slot, hid), F32)
    part = pltpu.VMEM((4, width, hid), BF16)
    half = pltpu.VMEM((n_col, hid, width), BF16)
    sums = pltpu.VMEM((2, n_slot, hid), F32)
    stacks = [far(w) for w in (swapped[0], swapped[1], params[0], params[1])]
    order = [0, 3, 1, 2]
    rows = [(held(got[0, d]), held(got[1, d])) for d in order]
    acc = pl.pallas_call(
        functools.partial(first_body, order[0]),
        name="step_a",
        in_specs=[smem] + [vmem] * 2 + [hbm] * 4,
        out_shape=four,
        out_specs=vmem,
        scratch_shapes=[part, pltpu.SemaphoreType.DMA((4,))],
        compiler_params=limit(8),
    )(blocks, *rows[0], *stacks)
    acc, high, low = lax.optimization_barrier((acc, high, low))
    acc, w1, w2, wn, wf = pl.pallas_call(
        functools.partial(second_body, order[1:]),
        name="step_b",
        in_specs=[smem] * 2 + [vmem] * 3 + [hbm] * 6,
        out_shape=[four, part, part, half, half],
        out_specs=[vmem] * 5,
        scratch_shapes=[part, pltpu.SemaphoreType.DMA((4,)), pltpu.SemaphoreType.DMA((8 + 2 * n_col,))],
        compiler_params=limit(8),
    )(blocks, b, *rows[1], held(acc), *stacks, far(params[2]), far(swapped[2]))
    acc = pl.pallas_call(
        third_body, name="step_c", in_specs=[vmem] * 4, out_shape=four, out_specs=vmem, compiler_params=limit(8)
    )(*rows[2], held(w1), held(acc))
    last = lambda at: pl.pallas_call(
        functools.partial(last_body, at), in_specs=[vmem] * 4, out_shape=sums, out_specs=vmem, compiler_params=limit(8)
    )(*rows[3], held(w2), held(acc))
    cross = lax.ppermute(last(0), "ba", swap)
    hidden = pl.pallas_call(
        hidden_body, name="hidden", out_shape=pltpu.VMEM((n_slot, hid), BF16), compiler_params=limit(8)
    )(held(last(2)), held(cross))
    other = lax.ppermute(hidden, "ba", swap)
    near = pl.pallas_call(
        near_body,
        name="near",
        out_shape=pltpu.VMEM((nh, ny, nx, n_col, CAP, width), F32),
        compiler_params=limit(8),
    )(held(hidden), held(wn))
    pair = pl.pallas_call(
        far_body,
        name="far",
        in_specs=[smem] + [vmem] * 3,
        out_shape=pltpu.VMEM((ny, nh, nx, n_col, CAP, width), BF16),
        compiler_params=limit(8),
    )(zh, held(other), held(wf), held(near))

    back = lax.all_to_all(pair.reshape(n_aa * n_col, CAP, width), axes, 0, 0, tiled=True)
    return pl.pallas_call(
        combine_body,
        out_shape=jax.ShapeDtypeStruct((n_tok, width), BF16),
        name="combine",
        compiler_params=limit(8),
    )(held(back.reshape(shape)), held(high), held(low))


def solution(mesh):
    in_specs = (
        P("aa", ("ba", "col")),
        P("aa", None),
        P("aa", None),
        P("aa", None, ("ba", "col")),
        P("aa", None, ("ba", "col")),
        P("aa", ("ba", "col"), None),
    )
    out_specs = P("aa", ("ba", "col"))
    return jax.shard_map(shards, mesh=mesh, in_specs=in_specs, out_specs=out_specs, check_vma=False)
```
